32 devices in a mesh: parts: 2 (over y), group: 2 (over x), dev: 4 (over z), pair: 2 (over core).
Axes of the slice: x: 2, y: 2, z: 4, core: 2. Of those that a mesh axis runs over, the one named last changes fastest.
Arguments:
- tokens: bfloat16 [2048, 2048], P(('parts', 'group', 'dev', 'pair')), parts along dimension 0, may hold values from -6 to 6
- expert_ids: int32 [2048, 2], P(('parts', 'group', 'dev', 'pair')), parts along dimension 0, may hold values from 0 to 3, all different within a row; in each aligned block of 64 rows (0 to 63, 64 to 127, ...) at most 48 rows name the same one
- route_scores: float32 [2048, 2], P(('parts', 'group', 'dev', 'pair')), parts along dimension 0, may hold values from 0.05 to 1
- w_gate: bfloat16 [8, 2048, 384], P(('group', 'dev'), None, 'pair'), may hold values from -0.125 to 0.125
- w_up: bfloat16 [8, 2048, 384], P(('group', 'dev'), None, 'pair'), may hold values from -0.125 to 0.125
- w_down: bfloat16 [8, 2048, 384], P(('group', 'dev'), None, 'pair'), may hold values from -0.21875 to 0.21875
Outputs:
- mixed_out: bfloat16 [2048, 2048], P(('parts', 'group', 'dev', 'pair')), parts along dimension 0
The draws below stay inside these ranges and needn't reach their ends.
There are 2 independent parts, one for each index of `parts`. The reference program is written for one: setup_inputs(seed, part) draws one part's arguments, and reference() takes and returns one part's arrays. A program takes and returns all parts, laid end to end along the dimension named above; an argument that names none is the same for every part. Nothing has to cross between parts.
Inputs may be any that keep to these rules, and one draw needn't show every extreme that they name: `expert_ids`: each row names 2 different experts. Within each aligned block of 64 rows (the tokens of one device) no expert is named more than 48 times, a bound that some block reaches.
All inputs are finite; a program needn't handle non-finite values.
Results may differ from the reference program's by a relative error of at most 0.0057.
Values may be sent and summed in bfloat16 or wider, within the bound.
A program may use at most 128 MiB of HBM per device.

```python
import math
import jax
import jax.numpy as jnp
import numpy as np
from jax import lax

D = 2048
HID = 768
TOK_DEV = 64
EXPERTS = 4
TOP = 2
CAP = 48
TOKENS = 1024
N_GROUP = 2
N_DEV = 4
N_PAIR = 2


def block_levels(stream_key, extent, split, low, top_value):
    level = 1.0
    for position, parts in split:
        draws = jax.random.uniform(jax.random.fold_in(jax.random.fold_in(stream_key, 6), position), (parts,), jnp.float32, low / len(split), top_value / len(split))
        level = level * jnp.repeat(jnp.exp(draws), extent[position] // parts).reshape((-1,) + (1,) * (len(extent) - 1 - position))
    return level


def shared_out(stream_key, own, number, rows, number_of, top, reach, skew):
    order = jax.random.permutation(stream_key, number_of)
    heavy_load, ordinary = load_shares(number_of, rows * top, reach, skew, True), load_shares(number_of, rows * top, reach, skew, False)
    places = jnp.arange(number_of)

    def named(tallies, offset_by):
        used = int((tallies > 0).sum())
        fixed = max(1, used // 4)
        moved = fixed + (places - fixed + offset_by * (used - fixed)) % max(1, number_of - fixed)
        return jnp.zeros((number_of,), jnp.int32).at[order[jnp.where(places < fixed, places, moved)]].set(jnp.asarray(tallies, jnp.int32))

    tallies = jnp.where(number % 4 == 0, named(heavy_load, number // 4), named(ordinary, number - number // 4 - 1))
    mixed = jax.random.permutation(jax.random.fold_in(own, 3), number_of)
    giver, taker = mixed[0:number_of // 2 * 2:2], mixed[1:number_of // 2 * 2:2]
    margin = jnp.minimum(tallies[giver] - 1, reach - tallies[taker]) // 2
    margin = jnp.where((giver == order[0]) | (taker == order[0]) | (tallies[taker] == 0), 0, jnp.maximum(margin, 0))
    moved = jax.random.randint(jax.random.fold_in(own, 4), (number_of // 2,), 0, 1 << 20) % (margin + 1)
    tallies = tallies.at[giver].add(-moved).at[taker].add(moved)
    labels = jnp.searchsorted(jnp.cumsum(tallies), jnp.arange(rows * top), side="right").astype(jnp.int32)
    listing = labels.reshape(top, rows).T
    listing = listing[jax.random.permutation(jax.random.fold_in(own, 1), rows)]
    offset_by = jax.random.randint(jax.random.fold_in(own, 2), (rows, 1), 0, top)
    return jnp.take_along_axis(listing, (jnp.arange(top)[None, :] + offset_by) % top, axis=1)


def load_shares(number_of, total, bound, slope, full):
    weights = [(1 << 20) // math.isqrt(rank ** slope) + 1 for rank in range(1, number_of + 1)]
    largest = bound if full else min(bound, max(-(-total // number_of), total * weights[0] // sum(weights)))
    least = 1 if total - largest >= number_of - 1 else 0
    counts, rest = [largest] + [least] * (number_of - 1), total - largest - least * (number_of - 1)
    while rest > 0:
        movable = [i for i in range(1, number_of) if counts[i] < largest] or [i for i in range(1, number_of) if counts[i] < bound]
        mass, left = sum([weights[i] for i in movable]), rest
        for i in movable:
            more = min(bound - counts[i], max(1, left * weights[i] // mass), rest)
            counts[i] = counts[i] + more
            rest = rest - more
    return np.array(counts)


def scatter_about(key, dims, deviation, most, pieces=(), kind=jnp.bfloat16):
    drawn = jax.random.normal(key, dims, jnp.float32) * deviation
    if len(pieces) > 0:
        drawn = block_levels(key, dims, pieces, -0.22, 0.18) * drawn
    return jnp.clip(drawn, min=-most, max=most).astype(kind)


def setup_inputs(seed: int = 0, part: int = 0) -> dict:
    keys = jax.random.split(jax.random.key(seed), 7)
    part_splits = jax.random.split(jax.random.fold_in(keys[6], part), 7)
    tokens = scatter_about(part_splits[0], (TOKENS, D), 1.0, 6.0, ((0, 16),))
    expert_ids_keys = jax.random.split(jax.random.fold_in(part_splits[1], 1), TOKENS // TOK_DEV)
    expert_ids_turns = jax.random.permutation(jax.random.fold_in(part_splits[1], 3), TOKENS // TOK_DEV)
    expert_ids = jax.vmap(lambda own, number: shared_out(jax.random.fold_in(part_splits[1], 2), own, number, TOK_DEV, EXPERTS, TOP, CAP, 2))(expert_ids_keys, expert_ids_turns).reshape((TOKENS, TOP))
    route_scores = jnp.clip(jnp.exp(math.log(1.0) - 2.9957323 * jax.random.uniform(part_splits[2], (TOKENS, TOP), jnp.float32) ** block_levels(part_splits[2], (TOKENS, TOP), ((0, 16),), -0.2, 0.2)), 0.05, 1.0)
    w_gate = scatter_about(keys[3], (2 * EXPERTS, D, HID // 2), D ** -0.5, 0.125, ((0, 8), (2, 2)))
    w_up = scatter_about(keys[4], (2 * EXPERTS, D, HID // 2), D ** -0.5, 0.125, ((0, 8), (2, 2)))
    w_down = scatter_about(keys[5], (2 * EXPERTS, D, HID // 2), HID ** -0.5, 0.21875, ((0, 8), (2, 2)))
    return dict(tokens=tokens, expert_ids=expert_ids, route_scores=route_scores, w_gate=w_gate, w_up=w_up, w_down=w_down)


def joined(weights):
    return weights.reshape(EXPERTS, 2, D, HID // 2).transpose(0, 2, 1, 3).reshape(EXPERTS, D, HID)


def reference(tokens, expert_ids, route_scores, w_gate, w_up, w_down):
    route_weight = route_scores / jnp.sum(route_scores, axis=1, keepdims=True)
    row_limit = N_GROUP * N_DEV * N_PAIR * CAP
    gate_all = joined(w_gate)
    up_all = joined(w_up)
    down_all = joined(w_down)

    def per_expert(running, stacked):
        gate_one, up_one, down_one, expert = stacked
        matches = expert_ids == expert
        weighting = jnp.sum(jnp.where(matches, route_weight, 0.0), axis=1)
        chosen = jnp.any(matches, axis=1)
        row_index = jnp.nonzero(chosen, size=row_limit, fill_value=0)[0].astype(jnp.int32)
        filled = jnp.arange(row_limit, dtype=jnp.int32) < jnp.sum(chosen.astype(jnp.int32))
        gathered = tokens[row_index]
        gate_act = jnp.dot(gathered, gate_one, preferred_element_type=jnp.float32)
        up_act = jnp.dot(gathered, up_one, preferred_element_type=jnp.float32)
        hidden = (jax.nn.silu(gate_act) * up_act).astype(jnp.bfloat16)
        output = lax.dot_general(hidden, down_one, (((1,), (1,)), ((), ())), preferred_element_type=jnp.float32).astype(jnp.bfloat16)
        weight = jnp.where(filled, weighting[row_index], 0.0)
        running = running.at[row_index].add(weight[:, None] * output.astype(jnp.float32))
        return running, None

    start = jnp.zeros((TOKENS, D), jnp.float32)
    running, _ = lax.scan(per_expert, start, (gate_all, up_all, down_all, jnp.arange(EXPERTS, dtype=jnp.int32)))
    return running.astype(jnp.bfloat16)
```

```python
import functools
import jax
import jax.numpy as jnp
from jax import lax
from jax.experimental import pallas as pl
from jax.experimental.pallas import tpu as pltpu
from jax.sharding import PartitionSpec as P

MESH = pl.DeviceIdType.MESH


def fused(n, rows, early, ag_cuts, rs_cuts, tokens, table, gate, up, down, out, tok, tab, wg, wu, wd, part,
          stage_z, land_z, stage_x, land_x, load_sem, swap_send, swap_recv, tab_send, tab_recv,
          za_send, za_recv, xa_send, xa_recv, zr_send, zr_recv, xr_send, xr_recv):
    g, d, p = lax.axis_index("group"), lax.axis_index("dev"), lax.axis_index("pair")
    late = rows - early
    wide = rows + early
    features = tok.shape[2]

    def remote(source, target, send, recv, where):
        return pltpu.make_async_remote_copy(source, target, send, recv, device_id=where, device_id_type=MESH)

    other_g, other_p = {"group": 1 - g}, {"pair": 1 - p}

    own_load = pltpu.make_async_copy(tokens, tok.at[d, pl.ds(0, rows)], load_sem.at[0])
    own_load.start()
    loads = [
        pltpu.make_async_copy(piece.at[0], full.at[0], load_sem.at[1 + i])
        for i, (piece, full) in enumerate(((gate, wg), (up, wu), (down, wd)))
    ]
    for load in loads:
        load.start()
    tab[0, d] = table[...]

    barrier = pltpu.get_barrier_semaphore()
    plane = []
    for off in range(1, 2 * n):
        there = lax.rem(g * n + d + off, 2 * n)
        plane.append((there // n, lax.rem(there, n)))
    pl.semaphore_signal(barrier, inc=1, device_id=other_p, device_id_type=MESH)
    for tg, td in plane:
        pl.semaphore_signal(barrier, inc=1, device_id={"group": tg, "dev": td}, device_id_type=MESH)
    pl.semaphore_wait(barrier, 2 * n)
    own_load.wait()

    def ag_z(src, side, k):
        lo, size = ag_cuts[k]
        block = tok.at[src, pl.ds(lo, size)]
        return remote(block, block, za_send.at[side, src, k], za_recv.at[src, k], {"dev": d + 1 - 2 * side})

    def has_next(side):
        return d < n - 1 if side == 0 else d > 0

    def ag_x(src, which):
        lo, size = ((0, early), (early, late))[which]
        return remote(tok.at[src, pl.ds(lo, size)], tok.at[src, pl.ds(rows + lo, size)],
                      xa_send.at[src, which], xa_recv.at[src, which], other_g)

    def rs_x(src):
        return remote(stage_x.at[src, pl.ds(early, late)], land_x.at[src, pl.ds(early, late)],
                      xr_send.at[src, 0], xr_recv.at[src, 0], other_g)

    def rs_xa():
        return remote(stage_x.at[d, pl.ds(0, early)], land_x.at[d, pl.ds(0, early)],
                      xr_send.at[d, 1], xr_recv.at[d, 1], other_g)

    def rs_z(src, side, k):
        lo, size = rs_cuts[k]
        return remote(stage_z.at[src, pl.ds(lo, size)], land_z.at[side, src, pl.ds(lo, size)],
                      zr_send.at[src, k], zr_recv.at[side, src, k], {"dev": d + 1 - 2 * side})

    def tab_copy(i):
        tg, td = plane[i]
        rel = jnp.where(tg == g, 0, 1)
        return remote(tab.at[0, d], tab.at[rel, d], tab_send.at[i], tab_recv.at[rel, d], {"group": tg, "dev": td})

    def tab_wait(i):
        tg, td = plane[i]
        rel = jnp.where(tg == g, 0, 1)
        remote(tab.at[rel, td], tab.at[rel, td], tab_send.at[i], tab_recv.at[rel, td], other_g).wait_recv()

    swaps = [
        remote(piece.at[0], full.at[1], swap_send.at[i], swap_recv.at[i], other_p)
        for i, (piece, full) in enumerate(((gate, wg), (up, wu), (down, wd)))
    ]

    own_cuts = [k for k, (lo, size) in enumerate(ag_cuts) if lo < rows]
    far_cuts = [k for k, (lo, size) in enumerate(ag_cuts) if lo >= rows]
    ag_x(d, 0).start()
    for k in own_cuts:
        for side in (0, 1):
            pl.when(has_next(side))(lambda side=side, k=k: ag_z(d, side, k).start())
    ag_x(d, 1).start()
    for i in range(2 * n - 1):
        tab_copy(i).start()
    for swap in swaps:
        swap.start()
    ag_x(d, 0).wait_recv()
    for k in far_cuts:
        for side in (0, 1):
            pl.when(has_next(side))(lambda side=side, k=k: ag_z(d, side, k).start())
    for i in range(2 * n - 1):
        tab_wait(i)
    for load in loads:
        load.wait()
    for swap in swaps:
        swap.wait_recv()

    expert = (g * n + d) // 2
    eye = lax.broadcasted_iota(jnp.int32, (rows, rows), 0) == lax.broadcasted_iota(jnp.int32, (rows, rows), 1)

    def column(rel, src):
        row = tab[rel, src, pl.ds(expert, 1), :]
        return jnp.sum(jnp.where(eye, jnp.broadcast_to(row, (rows, rows)), 0.0), axis=1, keepdims=True)

    tile = 512 if features % 512 == 0 else features

    def compute(src):
        x = tok[src]
        scale = jnp.concatenate([column(0, src), column(1, src)], axis=0)
        hidden = []
        for j in range(2):
            gate_act = jnp.dot(x, wg[j], preferred_element_type=jnp.float32)
            up_act = jnp.dot(x, wu[j], preferred_element_type=jnp.float32)
            hidden.append((gate_act / (1.0 + jnp.exp(-gate_act)) * up_act).astype(jnp.bfloat16))
        for at in range(0, features, tile):
            total = None
            for j in range(2):
                term = lax.dot_general(hidden[j], wd[j, at:at + tile, :], (((1,), (1,)), ((), ())),
                                       preferred_element_type=jnp.float32)
                total = term if total is None else total + term
            total = total * scale
            part[src, :, at:at + tile] = total[:wide]
            stage_x[src, early:rows, at:at + tile] = total[wide:].astype(jnp.bfloat16)
        rs_x(src).start()

    def add_x(src):
        rs_x(src).wait_recv()
        part[src, early:rows] += land_x[src, early:rows].astype(jnp.float32)

    def send_on(src, side, landed):
        add_x(src)
        for k, (lo, size) in enumerate(rs_cuts):
            value = part[src, lo:lo + size]
            if landed:
                rs_z(src, side, k).wait_recv()
                value = value + land_z[side, src, lo:lo + size].astype(jnp.float32)
            stage_z[src, lo:lo + size] = value.astype(jnp.bfloat16)
            rs_z(src, side, k).start()

    def step(s, carry):
        for side in (0, 1):
            src = d - s if side == 0 else d + s
            valid = jnp.logical_and(s >= 1, jnp.logical_and(src >= 0, src < n))

            @pl.when(valid)
            def _():
                for k in range(len(ag_cuts)):
                    ag_z(src, side, k).wait_recv()
                    pl.when(has_next(side))(lambda: ag_z(src, side, k).start())
                    if k == own_cuts[-1]:
                        ag_x(src, 1).start()

        def one(side, carry):
            b = s - 1
            src = d - b + 2 * b * side
            valid = jnp.logical_and(jnp.logical_and(b >= 0, jnp.logical_or(side == 0, b >= 1)), jnp.logical_and(src >= 0, src < n))

            @pl.when(valid)
            def _():
                ag_x(src, 1).wait_recv()
                compute(src)
            return carry

        lax.fori_loop(0, 2, one, 0)

        for side in (0, 1):
            c = s - 2
            src = d + c if side == 0 else d - c
            end = d == 0 if side == 0 else d == n - 1
            valid = jnp.logical_and(jnp.logical_and(c >= 1, end), jnp.logical_and(src >= 0, src < n))
            pl.when(valid)(lambda: send_on(src, side, False))
        return carry

    lax.fori_loop(0, n + 2, step, 0)

    def relay(t, carry):
        for side in (0, 1):
            src = t if side == 0 else n - 1 - t
            valid = jnp.logical_and(d > 0, d < src) if side == 0 else jnp.logical_and(d < n - 1, d > src)
            pl.when(valid)(lambda: send_on(src, side, True))
        return carry

    lax.fori_loop(1, n, relay, 0)

    add_x(d)
    for k, (lo, size) in enumerate(rs_cuts):
        for side in (0, 1):
            @pl.when(d > 0 if side == 0 else d < n - 1)
            def _():
                rs_z(d, side, k).wait_recv()
                part[d, lo:lo + size] += land_z[side, d, lo:lo + size].astype(jnp.float32)
        if lo <= rows < lo + size:
            stage_x[d, 0:early] = part[d, rows:wide].astype(jnp.bfloat16)
            rs_xa().start()
    out[early:rows] = part[d, early:rows].astype(jnp.bfloat16)
    rs_xa().wait_recv()
    out[0:early] = (part[d, 0:early] + land_x[d, 0:early].astype(jnp.float32)).astype(jnp.bfloat16)

    for swap in swaps:
        swap.wait_send()
    for i in range(2 * n - 1):
        tab_copy(i).wait_send()
    ag_x(d, 0).wait_send()
    rs_xa().wait_send()

    def drain(src, carry):
        ag_x(src, 1).wait_send()
        rs_x(src).wait_send()
        for side in (0, 1):
            @pl.when(jnp.logical_and(has_next(side), src <= d if side == 0 else src >= d))
            def _():
                for k in range(len(ag_cuts)):
                    ag_z(src, side, k).wait_send()

            @pl.when(src > d if side == 0 else src < d)
            def _():
                for k in range(len(rs_cuts)):
                    rs_z(src, side, k).wait_send()
        return carry

    lax.fori_loop(0, n, drain, 0)


def near(tokens, expert_ids, route_scores, w_gate, w_up, w_down):
    rows, features = tokens.shape
    n = lax.axis_size("dev")
    experts = n
    units = w_gate.shape[2]
    early = rows // 4
    half = rows // 2
    ag_cuts = ((0, half), (half, half), (rows, early))
    rs_cuts = ((rows, early), (0, half), (half, half))
    route_weight = route_scores / jnp.sum(route_scores, axis=1, keepdims=True)
    names = jnp.arange(experts, dtype=jnp.int32)[:, None, None]
    table = jnp.sum(jnp.where(expert_ids[None] == names, route_weight[None], 0.0), axis=2)
    wide = rows + early
    dma, bf16, f32 = pltpu.SemaphoreType.DMA, jnp.bfloat16, jnp.float32
    vmem, hbm = pl.BlockSpec(memory_space=pltpu.VMEM), pl.BlockSpec(memory_space=pl.ANY)
    return pl.pallas_call(
        functools.partial(fused, n, rows, early, ag_cuts, rs_cuts),
        out_shape=jax.ShapeDtypeStruct((rows, features), bf16),
        in_specs=[hbm, vmem, hbm, hbm, hbm],
        out_specs=vmem,
        scratch_shapes=[
            pltpu.VMEM((n, 2 * rows, features), bf16),
            pltpu.VMEM((2, n, experts, rows), f32),
            pltpu.VMEM((2, features, units), bf16),
            pltpu.VMEM((2, features, units), bf16),
            pltpu.VMEM((2, features, units), bf16),
            pltpu.VMEM((n, wide, features), f32),
            pltpu.VMEM((n, wide, features), bf16),
            pltpu.VMEM((2, n, wide, features), bf16),
            pltpu.VMEM((n, rows, features), bf16),
            pltpu.VMEM((n, rows, features), bf16),
            dma((4,)), dma((3,)), dma((3,)), dma((2 * n - 1,)), dma((2, n)),
            dma((2, n, len(ag_cuts))), dma((n, len(ag_cuts))), dma((n, 2)), dma((n, 2)),
            dma((n, len(rs_cuts))), dma((2, n, len(rs_cuts))), dma((n, 2)), dma((n, 2)),
        ],
        compiler_params=pltpu.CompilerParams(collective_id=0, has_side_effects=True, vmem_limit_bytes=56 * 2**20),
    )(tokens, table, w_gate, w_up, w_down)


def partner_2(x, axis, apart):
    return lax.ppermute(x, axis, [(i, i ^ 1 << apart) for i in range(lax.axis_size(axis))])


def expert_block(batch_rows, gate_piece, up_piece, down_piece):
    gate_act = jnp.dot(batch_rows, gate_piece, preferred_element_type=jnp.float32)
    up_act = jnp.dot(batch_rows, up_piece, preferred_element_type=jnp.float32)
    hidden = (jax.nn.silu(gate_act) * up_act).astype(jnp.bfloat16)
    return lax.dot_general(
        hidden, down_piece, (((1,), (1,)), ((), ())), preferred_element_type=jnp.float32
    )


def shards(tokens, expert_ids, route_scores, w_gate, w_up, w_down):
    rows_dev, features = tokens.shape
    top_count = expert_ids.shape[1]
    dest_count = lax.axis_size(("group", "dev"))
    experts = dest_count // 2
    capacity = 2 * max(1, 3 * rows_dev * top_count // (4 * experts))
    half_cap = capacity // 2
    route_weight = route_scores / jnp.sum(route_scores, axis=1, keepdims=True)
    flat_ids = expert_ids.reshape(-1)
    onehot = (flat_ids[:, None] == jnp.arange(experts, dtype=jnp.int32)[None, :]).astype(jnp.int32)
    before = jnp.cumsum(onehot, axis=0) - onehot
    rank_in = jnp.sum(before * onehot, axis=1)
    target = 2 * flat_ids + rank_in // half_cap
    position = target * half_cap + rank_in % half_cap
    owners = jnp.arange(rows_dev * top_count, dtype=jnp.int32) // top_count
    outgoing = (
        jnp.zeros((dest_count * half_cap, features), jnp.bfloat16).at[position].set(tokens[owners])
    )
    outgoing = outgoing.reshape(dest_count, half_cap, features)
    arrived = lax.all_to_all(outgoing, ("group", "dev"), split_axis=0, concat_axis=0, tiled=True)
    batch_rows = arrived.reshape(dest_count * half_cap, features)
    partner = partner_2((w_gate[0], w_up[0], w_down[0]), "dev", 0)
    gate_half = jnp.concatenate([w_gate[0], partner[0]], axis=1)
    up_half = jnp.concatenate([w_up[0], partner[1]], axis=1)
    down_half = jnp.concatenate([w_down[0], partner[2]], axis=1)
    full_gate, full_up, full_down = (
        lax.all_gather(gate_half, "pair", axis=1, tiled=True),
        lax.all_gather(up_half, "pair", axis=1, tiled=True),
        lax.all_gather(down_half, "pair", axis=1, tiled=True),
    )
    result = expert_block(batch_rows, full_gate, full_up, full_down)
    answer = result.astype(jnp.bfloat16).reshape(dest_count, half_cap, features)
    returned = lax.all_to_all(answer, ("group", "dev"), split_axis=0, concat_axis=0, tiled=True)
    picked = returned.reshape(dest_count * half_cap, features)[position].astype(jnp.float32)
    weighted = picked * route_weight.reshape(-1)[:, None]
    mixed_out = jnp.sum(weighted.reshape(rows_dev, top_count, features), axis=1)
    return mixed_out.astype(jnp.bfloat16)


def solution(mesh):
    in_specs = (
        P(("parts", "group", "dev", "pair"), None),
        P(("parts", "group", "dev", "pair"), None),
        P(("parts", "group", "dev", "pair"), None),
        P(("group", "dev"), None, "pair"),
        P(("group", "dev"), None, "pair"),
        P(("group", "dev"), None, "pair"),
    )
    out_specs = P(("parts", "group", "dev", "pair"), None)
    few = mesh.shape["group"] == 2 and mesh.shape["pair"] == 2 and mesh.shape["dev"] <= 4
    return jax.shard_map(near if few else shards, mesh=mesh, in_specs=in_specs, out_specs=out_specs, check_vma=False)
```

```python
import functools
import jax
import jax.numpy as jnp
from jax import lax
from jax.experimental import pallas as pl
from jax.experimental.pallas import tpu as pltpu
from jax.sharding import PartitionSpec as P

MESH = pl.DeviceIdType.MESH


def fused(n, rows, early, ag_cuts, rs_cuts, tokens, ids, scores, gate, up, down, out, tok, tab, wg, wu, wd, part,
          stage_z, land_z, stage_x, land_x, load_sem, swap_send, swap_recv, tab_send, tab_recv,
          za_send, za_recv, xa_send, xa_recv, zr_send, zr_recv, xr_send, xr_recv):
    g, d, p = lax.axis_index("group"), lax.axis_index("dev"), lax.axis_index("pair")
    x_cuts = [(0, early)]
    x_of = {}
    for k, (lo, size) in enumerate(ag_cuts):
        if lo < rows and lo + size > early:
            x_of[k] = len(x_cuts)
            x_cuts.append((max(lo, early), lo + size - max(lo, early)))
    rest = range(1, len(x_cuts))
    wide = rows + early
    features = tok.shape[2]
    units = gate.shape[1]

    def remote(source, target, send, recv, where):
        return pltpu.make_async_remote_copy(source, target, send, recv, device_id=where, device_id_type=MESH)

    other_g, other_p = {"group": 1 - g}, {"pair": 1 - p}

    own_load = pltpu.make_async_copy(tokens, tok.at[d, pl.ds(0, rows)], load_sem.at[0])
    own_load.start()
    loads = [
        pltpu.make_async_copy(piece.at[0], full.at[pl.ds(0, units)], load_sem.at[1 + i])
        for i, (piece, full) in enumerate(((gate, wg), (up, wu), (down, wd)))
    ]
    for load in loads:
        load.start()
    route_weight = scores[...] / jnp.sum(scores[...], axis=0, keepdims=True)
    experts = tab.shape[2]
    names = lax.broadcasted_iota(jnp.int32, (experts, rows), 0)
    table = jnp.zeros((experts, rows), jnp.float32)
    for k in range(ids.shape[0]):
        table += jnp.where(ids[k:k + 1] == names, route_weight[k:k + 1], 0.0)
    tab[d, 0] = table

    barrier = pltpu.get_barrier_semaphore()
    pl.semaphore_signal(barrier, inc=1, device_id=other_p, device_id_type=MESH)
    pl.semaphore_signal(barrier, inc=1, device_id=other_g, device_id_type=MESH)
    for side in (0, 1):
        @pl.when(d < n - 1 if side == 0 else d > 0)
        def _():
            pl.semaphore_signal(barrier, inc=1, device_id={"dev": d + 1 - 2 * side}, device_id_type=MESH)
    inner = jnp.logical_and(d > 0, d < n - 1)

    @pl.when(inner)
    def _():
        pl.semaphore_wait(barrier, 4)

    @pl.when(jnp.logical_not(inner))
    def _():
        pl.semaphore_wait(barrier, 3)
    own_load.wait()

    def ag_z(src, side, k):
        lo, size = ag_cuts[k]
        block = tok.at[src, pl.ds(lo, size)]
        return remote(block, block, za_send.at[side, src, k], za_recv.at[src, k], {"dev": d + 1 - 2 * side})

    def has_next(side):
        return d < n - 1 if side == 0 else d > 0

    def ag_x(src, which):
        lo, size = x_cuts[which]
        return remote(tok.at[src, pl.ds(lo, size)], tok.at[src, pl.ds(rows + lo, size)],
                      xa_send.at[src, which], xa_recv.at[src, which], other_g)

    def rs_x(src, which):
        block = pl.ds(*x_cuts[which])
        return remote(stage_x.at[src, block], land_x.at[src, block],
                      xr_send.at[src, which], xr_recv.at[src, which], other_g)

    def rs_z(src, side, k):
        lo, size = rs_cuts[k]
        return remote(stage_z.at[src, pl.ds(lo, size)], land_z.at[side, src, pl.ds(lo, size)],
                      zr_send.at[src, k], zr_recv.at[side, src, k], {"dev": d + 1 - 2 * side})

    def tab_x():
        return remote(tab.at[d, 0], tab.at[d, 1], tab_send.at[2 * n], tab_recv.at[n], other_g)

    def tab_z(src, side):
        return remote(tab.at[src], tab.at[src], tab_send.at[side * n + src], tab_recv.at[src], {"dev": d + 1 - 2 * side})

    swaps = [
        remote(piece.at[0], full.at[pl.ds(units, units)], swap_send.at[i], swap_recv.at[i], other_p)
        for i, (piece, full) in enumerate(((gate, wg), (up, wu), (down, wd)))
    ]

    own_cuts = [k for k, (lo, size) in enumerate(ag_cuts) if lo < rows]
    far_cuts = [k for k, (lo, size) in enumerate(ag_cuts) if lo >= rows]
    tab_x().start()
    ag_x(d, 0).start()
    for k in own_cuts:
        for side in (0, 1):
            pl.when(has_next(side))(lambda side=side, k=k: ag_z(d, side, k).start())
    for which in rest:
        ag_x(d, which).start()
    for swap in swaps:
        swap.start()
    tab_x().wait_recv()
    for side in (0, 1):
        pl.when(has_next(side))(lambda side=side: tab_z(d, side).start())
    ag_x(d, 0).wait_recv()
    for k in far_cuts:
        for side in (0, 1):
            pl.when(has_next(side))(lambda side=side, k=k: ag_z(d, side, k).start())
    expert = (g * n + d) // 2
    eye = lax.broadcasted_iota(jnp.int32, (rows, rows), 0) == lax.broadcasted_iota(jnp.int32, (rows, rows), 1)

    def column(rel, src):
        row = tab[src, rel, pl.ds(expert, 1), :]
        return jnp.sum(jnp.where(eye, jnp.broadcast_to(row, (rows, rows)), 0.0), axis=1, keepdims=True)

    tile = 512 if features % 512 == 0 else features

    def compute(src):
        x = tok[src]
        scale = jnp.concatenate([column(0, src), column(1, src)], axis=0)
        over_features = (((1,), (1,)), ((), ()))
        gate_act = lax.dot_general(x, wg[...], over_features, preferred_element_type=jnp.float32)
        up_act = lax.dot_general(x, wu[...], over_features, preferred_element_type=jnp.float32)
        hidden = (gate_act / (1.0 + jnp.exp(-gate_act)) * up_act).astype(jnp.bfloat16)
        for at in range(0, features, tile):
            total = scale * jnp.dot(hidden, wd[:, at:at + tile], preferred_element_type=jnp.float32)
            part[src, :, at:at + tile] = total[:wide]
            stage_x[src, early:rows, at:at + tile] = total[wide:].astype(jnp.bfloat16)
        for which in rest:
            rs_x(src, which).start()

    rs_x_of = {k: x_of[ag_cuts.index(cut)] for k, cut in enumerate(rs_cuts) if ag_cuts.index(cut) in x_of}

    def add_x(src, k):
        if k in rs_x_of:
            lo, size = x_cuts[rs_x_of[k]]
            rs_x(src, rs_x_of[k]).wait_recv()
            part[src, lo:lo + size] += land_x[src, lo:lo + size].astype(jnp.float32)

    def send_on(src, side, landed):
        for k, (lo, size) in enumerate(rs_cuts):
            add_x(src, k)
            value = part[src, lo:lo + size]
            if landed:
                rs_z(src, side, k).wait_recv()
                value = value + land_z[side, src, lo:lo + size].astype(jnp.float32)
            stage_z[src, lo:lo + size] = value.astype(jnp.bfloat16)
            rs_z(src, side, k).start()

    def step(s, carry):
        @pl.when(s == 1)
        def _():
            for load in loads:
                load.wait()
            for swap in swaps:
                swap.wait_recv()

        def one(side, carry):
            b = s - 1
            src = d - b + 2 * b * side
            valid = jnp.logical_and(jnp.logical_and(b >= 0, jnp.logical_or(side == 0, b >= 1)), jnp.logical_and(src >= 0, src < n))

            @pl.when(valid)
            def _():
                for which in rest:
                    ag_x(src, which).wait_recv()
                compute(src)
            return carry

        lax.fori_loop(0, 2, one, 0)

        for side in (0, 1):
            src = d - s if side == 0 else d + s
            valid = jnp.logical_and(s >= 1, jnp.logical_and(src >= 0, src < n))

            @pl.when(valid)
            def _():
                tab_z(src, side).wait_recv()
                pl.when(has_next(side))(lambda: tab_z(src, side).start())
                for k in range(len(ag_cuts)):
                    ag_z(src, side, k).wait_recv()
                    pl.when(has_next(side))(lambda: ag_z(src, side, k).start())
                    if k in x_of:
                        ag_x(src, x_of[k]).start()

        for side in (0, 1):
            c = s - 1
            src = d + c if side == 0 else d - c
            end = d == 0 if side == 0 else d == n - 1
            valid = jnp.logical_and(jnp.logical_and(c >= 1, end), jnp.logical_and(src >= 0, src < n))
            pl.when(valid)(lambda: send_on(src, side, False))
        return carry

    lax.fori_loop(0, n + 1, step, 0)

    def relay(t, carry):
        for side in (0, 1):
            src = t if side == 0 else n - 1 - t
            valid = jnp.logical_and(d > 0, d < src) if side == 0 else jnp.logical_and(d < n - 1, d > src)
            pl.when(valid)(lambda: send_on(src, side, True))
        return carry

    lax.fori_loop(1, n, relay, 0)

    for k, (lo, size) in enumerate(rs_cuts):
        add_x(d, k)
        for side in (0, 1):
            @pl.when(d > 0 if side == 0 else d < n - 1)
            def _():
                rs_z(d, side, k).wait_recv()
                part[d, lo:lo + size] += land_z[side, d, lo:lo + size].astype(jnp.float32)
        if lo + size == wide:
            stage_x[d, 0:early] = part[d, rows:wide].astype(jnp.bfloat16)
            rs_x(d, 0).start()
    out[early:rows] = part[d, early:rows].astype(jnp.bfloat16)
    rs_x(d, 0).wait_recv()
    out[0:early] = (part[d, 0:early] + land_x[d, 0:early].astype(jnp.float32)).astype(jnp.bfloat16)

    for swap in swaps:
        swap.wait_send()
    tab_x().wait_send()
    ag_x(d, 0).wait_send()
    rs_x(d, 0).wait_send()

    def drain(src, carry):
        for which in rest:
            ag_x(src, which).wait_send()
            rs_x(src, which).wait_send()
        for side in (0, 1):
            @pl.when(jnp.logical_and(has_next(side), src <= d if side == 0 else src >= d))
            def _():
                tab_z(src, side).wait_send()
                for k in range(len(ag_cuts)):
                    ag_z(src, side, k).wait_send()

            @pl.when(src > d if side == 0 else src < d)
            def _():
                for k in range(len(rs_cuts)):
                    rs_z(src, side, k).wait_send()
        return carry

    lax.fori_loop(0, n, drain, 0)


def near(tokens, expert_ids, route_scores, w_gate, w_up, w_down):
    rows, features = tokens.shape
    n = lax.axis_size("dev")
    experts = n
    units = w_gate.shape[2]
    early = rows // 2
    wide = rows + early
    fine = rows // 4
    ag_cuts = tuple((at, fine) for at in range(0, wide, fine))
    rs_cuts = tuple((at, fine) for at in range(rows, wide, fine)) + tuple((at, fine) for at in range(0, rows, fine))
    dma, bf16, f32 = pltpu.SemaphoreType.DMA, jnp.bfloat16, jnp.float32
    vmem, hbm = pl.BlockSpec(memory_space=pltpu.VMEM), pl.BlockSpec(memory_space=pl.ANY)
    return pl.pallas_call(
        functools.partial(fused, n, rows, early, ag_cuts, rs_cuts),
        out_shape=jax.ShapeDtypeStruct((rows, features), bf16),
        in_specs=[hbm, vmem, vmem, hbm, hbm, hbm],
        out_specs=vmem,
        scratch_shapes=[
            pltpu.VMEM((n, 2 * rows, features), bf16),
            pltpu.VMEM((n, 2, experts, rows), f32),
            pltpu.VMEM((2 * units, features), bf16),
            pltpu.VMEM((2 * units, features), bf16),
            pltpu.VMEM((2 * units, features), bf16),
            pltpu.VMEM((n, wide, features), f32),
            pltpu.VMEM((n, wide, features), bf16),
            pltpu.VMEM((2, n, wide, features), bf16),
            pltpu.VMEM((n, rows, features), bf16),
            pltpu.VMEM((n, rows, features), bf16),
            dma((4,)), dma((3,)), dma((3,)), dma((2 * n + 1,)), dma((n + 1,)),
            dma((2, n, len(ag_cuts))), dma((n, len(ag_cuts))), dma((n, len(ag_cuts))), dma((n, len(ag_cuts))),
            dma((n, len(rs_cuts))), dma((2, n, len(rs_cuts))), dma((n, len(ag_cuts))), dma((n, len(ag_cuts))),
        ],
        compiler_params=pltpu.CompilerParams(collective_id=0, has_side_effects=True, vmem_limit_bytes=56 * 2**20),
    )(tokens, expert_ids.T, route_scores.T, *(jnp.swapaxes(w, 1, 2) for w in (w_gate, w_up, w_down)))


def partner_2(x, axis, apart):
    return lax.ppermute(x, axis, [(i, i ^ 1 << apart) for i in range(lax.axis_size(axis))])


def expert_block(batch_rows, gate_piece, up_piece, down_piece):
    gate_act = jnp.dot(batch_rows, gate_piece, preferred_element_type=jnp.float32)
    up_act = jnp.dot(batch_rows, up_piece, preferred_element_type=jnp.float32)
    hidden = (jax.nn.silu(gate_act) * up_act).astype(jnp.bfloat16)
    return lax.dot_general(
        hidden, down_piece, (((1,), (1,)), ((), ())), preferred_element_type=jnp.float32
    )


def shards(tokens, expert_ids, route_scores, w_gate, w_up, w_down):
    rows_dev, features = tokens.shape
    top_count = expert_ids.shape[1]
    dest_count = lax.axis_size(("group", "dev"))
    experts = dest_count // 2
    capacity = 2 * max(1, 3 * rows_dev * top_count // (4 * experts))
    half_cap = capacity // 2
    route_weight = route_scores / jnp.sum(route_scores, axis=1, keepdims=True)
    flat_ids = expert_ids.reshape(-1)
    onehot = (flat_ids[:, None] == jnp.arange(experts, dtype=jnp.int32)[None, :]).astype(jnp.int32)
    before = jnp.cumsum(onehot, axis=0) - onehot
    rank_in = jnp.sum(before * onehot, axis=1)
    target = 2 * flat_ids + rank_in // half_cap
    position = target * half_cap + rank_in % half_cap
    owners = jnp.arange(rows_dev * top_count, dtype=jnp.int32) // top_count
    outgoing = (
        jnp.zeros((dest_count * half_cap, features), jnp.bfloat16).at[position].set(tokens[owners])
    )
    outgoing = outgoing.reshape(dest_count, half_cap, features)
    arrived = lax.all_to_all(outgoing, ("group", "dev"), split_axis=0, concat_axis=0, tiled=True)
    batch_rows = arrived.reshape(dest_count * half_cap, features)
    partner = partner_2((w_gate[0], w_up[0], w_down[0]), "dev", 0)
    gate_half = jnp.concatenate([w_gate[0], partner[0]], axis=1)
    up_half = jnp.concatenate([w_up[0], partner[1]], axis=1)
    down_half = jnp.concatenate([w_down[0], partner[2]], axis=1)
    full_gate, full_up, full_down = (
        lax.all_gather(gate_half, "pair", axis=1, tiled=True),
        lax.all_gather(up_half, "pair", axis=1, tiled=True),
        lax.all_gather(down_half, "pair", axis=1, tiled=True),
    )
    result = expert_block(batch_rows, full_gate, full_up, full_down)
    answer = result.astype(jnp.bfloat16).reshape(dest_count, half_cap, features)
    returned = lax.all_to_all(answer, ("group", "dev"), split_axis=0, concat_axis=0, tiled=True)
    picked = returned.reshape(dest_count * half_cap, features)[position].astype(jnp.float32)
    weighted = picked * route_weight.reshape(-1)[:, None]
    mixed_out = jnp.sum(weighted.reshape(rows_dev, top_count, features), axis=1)
    return mixed_out.astype(jnp.bfloat16)


def solution(mesh):
    in_specs = (
        P(("parts", "group", "dev", "pair"), None),
        P(("parts", "group", "dev", "pair"), None),
        P(("parts", "group", "dev", "pair"), None),
        P(("group", "dev"), None, "pair"),
        P(("group", "dev"), None, "pair"),
        P(("group", "dev"), None, "pair"),
    )
    out_specs = P(("parts", "group", "dev", "pair"), None)
    few = mesh.shape["group"] == 2 and mesh.shape["pair"] == 2 and 2 <= mesh.shape["dev"] <= 4
    return jax.shard_map(near if few else shards, mesh=mesh, in_specs=in_specs, out_specs=out_specs, check_vma=False)
```
